8 devices in a mesh: data: 8 (over z, y, x, core).
Axes of the slice: x: 2, y: 2, z: 1, core: 2. Of those that a mesh axis runs over, the one named last changes fastest.
Arguments:
- x_init: bfloat16 [256, 128, 768], P('data')
- cot_out: bfloat16 [256, 128, 768], P('data')
- w_query: bfloat16 [6, 768, 768], replicated
- w_key: bfloat16 [6, 768, 768], replicated
- w_value: bfloat16 [6, 768, 768], replicated
- w_proj: bfloat16 [6, 768, 768], replicated
- w_up: bfloat16 [768, 3072], replicated
- w_down: bfloat16 [3072, 768], replicated
Outputs:
- output 1: float32 [6, 768, 768], replicated
- output 2: float32 [6, 768, 768], replicated
- output 3: float32 [6, 768, 768], replicated
- output 4: float32 [6, 768, 768], replicated
- output 5: float32 [768, 3072], replicated
- output 6: float32 [3072, 768], replicated
- output 7: bfloat16 [256, 128, 768], P('data')
All inputs are finite; a program needn't handle non-finite values.
Results may differ from the reference program's by a relative error of at most 0.02.
Values are sent between devices in bfloat16 or wider.
A program may use at most 1 GiB of HBM per device.

```python
import jax
import jax.numpy as jnp
from jax import lax

D = 768
HEADS = 12
LAYERS = 6
BATCH = 256
SEQ = 128
FF = 4 * D
HEAD_DIM = D // HEADS
EPS = 1e-6


def setup_inputs(seed: int = 0) -> dict:
    keys = jax.random.split(jax.random.key(seed), 8)
    res_scale = (2.0 * LAYERS) ** -0.5
    x_init = jax.random.normal(keys[0], (BATCH, SEQ, D), jnp.float32)
    cot_out = jax.random.normal(keys[1], (BATCH, SEQ, D), jnp.float32)
    w_query = jax.random.normal(keys[2], (LAYERS, D, D), jnp.float32) * D ** -0.5
    w_key = jax.random.normal(keys[3], (LAYERS, D, D), jnp.float32) * D ** -0.5
    w_value = jax.random.normal(keys[4], (LAYERS, D, D), jnp.float32) * D ** -0.5
    w_proj = jax.random.normal(keys[5], (LAYERS, D, D), jnp.float32) * (D ** -0.5 * res_scale)
    w_up = jax.random.normal(keys[6], (D, FF), jnp.float32) * D ** -0.5
    w_down = jax.random.normal(keys[7], (FF, D), jnp.float32) * (FF ** -0.5 * res_scale)
    return {
        "x_init": x_init.astype(jnp.bfloat16),
        "cot_out": cot_out.astype(jnp.bfloat16),
        "w_query": w_query.astype(jnp.bfloat16),
        "w_key": w_key.astype(jnp.bfloat16),
        "w_value": w_value.astype(jnp.bfloat16),
        "w_proj": w_proj.astype(jnp.bfloat16),
        "w_up": w_up.astype(jnp.bfloat16),
        "w_down": w_down.astype(jnp.bfloat16),
    }


def rms_norm(x_f32):
    return x_f32 * lax.rsqrt(jnp.mean(x_f32 * x_f32, axis=-1, keepdims=True) + EPS)


def as_bf16(val_f32):
    return val_f32.astype(jnp.bfloat16).astype(jnp.float32)


def layer_fwd(x_seq, w_query, w_key, w_value, w_proj, w_up, w_down):
    x_f32 = x_seq.astype(jnp.float32)
    normed = as_bf16(rms_norm(x_f32))
    query = as_bf16(jnp.dot(normed, w_query, preferred_element_type=jnp.float32)).reshape(SEQ, HEADS, HEAD_DIM)
    key_act = as_bf16(jnp.dot(normed, w_key, preferred_element_type=jnp.float32)).reshape(SEQ, HEADS, HEAD_DIM)
    value = as_bf16(jnp.dot(normed, w_value, preferred_element_type=jnp.float32)).reshape(SEQ, HEADS, HEAD_DIM)
    scores = jnp.einsum("qhd,khd->hqk", query, key_act) * HEAD_DIM ** -0.5
    probs = as_bf16(jax.nn.softmax(scores, axis=-1))
    mixed = as_bf16(jnp.einsum("hqk,khd->qhd", probs, value)).reshape(SEQ, D)
    hidden = as_bf16(x_f32 + as_bf16(jnp.dot(mixed, w_proj, preferred_element_type=jnp.float32)))
    normed2 = as_bf16(rms_norm(hidden))
    pre_act = as_bf16(jnp.dot(normed2, w_up, preferred_element_type=jnp.float32))
    activated = as_bf16(jax.nn.gelu(pre_act, approximate=True))
    mlp_out = as_bf16(jnp.dot(activated, w_down, preferred_element_type=jnp.float32))
    return (hidden + mlp_out).astype(jnp.bfloat16)


layer_ckpt = jax.checkpoint(layer_fwd)


def stack_fwd(x_seq, w_query, w_key, w_value, w_proj, w_up, w_down):
    def layer_step(x_carry, layer_w):
        x_new = layer_ckpt(x_carry, layer_w[0], layer_w[1], layer_w[2], layer_w[3], w_up, w_down)
        return x_new, None

    return lax.scan(layer_step, x_seq, (w_query, w_key, w_value, w_proj))[0]


def reference(x_init, cot_out, w_query, w_key, w_value, w_proj, w_up, w_down):
    weights = (
        w_query.astype(jnp.float32),
        w_key.astype(jnp.float32),
        w_value.astype(jnp.float32),
        w_proj.astype(jnp.float32),
        w_up.astype(jnp.float32),
        w_down.astype(jnp.float32),
    )
    zero_sums = tuple(jnp.zeros_like(weight) for weight in weights)

    def per_sequence(grad_sums, seq_pair):
        pull_back = jax.vjp(stack_fwd, seq_pair[0], *weights)[1]
        seq_grads = pull_back(seq_pair[1])
        new_sums = tuple(total + part for total, part in zip(grad_sums, seq_grads[1:]))
        return new_sums, seq_grads[0]

    grad_sums, dx_init = lax.scan(per_sequence, zero_sums, (x_init, cot_out))
    return (grad_sums[0], grad_sums[1], grad_sums[2], grad_sums[3], grad_sums[4], grad_sums[5], dx_init)
```

```python
import functools

import jax
import jax.numpy as jnp
from jax import lax
from jax.experimental import pallas as pl
from jax.experimental.pallas import tpu as pltpu
from jax.sharding import PartitionSpec as P

EPS = 1e-6
HEAD_DIM = 64
BF = jnp.bfloat16
F32 = jnp.float32
SEQ = 128
PAIR = 2 * HEAD_DIM
SCALE = HEAD_DIM ** -0.5
LOG2E = 1.4426950408889634
GC = 0.7978845608028654
GA = 0.044715


def mm(a, b, ca=1, cb=0):
    return lax.dot_general(a, b, (((ca,), (cb,)), ((), ())), preferred_element_type=F32)


def inv_rms(v):
    return lax.rsqrt(jnp.mean(v * v, axis=-1, keepdims=True) + EPS)


def stack_heads(val):
    lane = lax.broadcasted_iota(jnp.int32, val.shape, 1)
    zero = jnp.zeros_like(val)
    return jnp.concatenate([jnp.where(lane < HEAD_DIM, val, zero), jnp.where(lane < HEAD_DIM, zero, val)], axis=0)


def rows_of(val):
    return jnp.concatenate([val[:, :SEQ], val[:, SEQ:]], axis=0)


def gelu(x):
    t = jnp.tanh(x * (GC + (GC * GA) * (x * x)))
    h = 0.5 * x
    return h + h * t


def fwd_body(x_ref, wq, wk, wv, wo, w1, w2, xs_o, q_o, k_o, v_o, p_o, mix_o, hid_o, n2_o, pre_o, act_o, xbuf, *, layers, tb):
    layer = pl.program_id(0)
    rows = pl.ds(pl.multiple_of(pl.program_id(1) * tb, tb), tb)
    pairs = q_o.shape[-1] // PAIR

    @pl.when(layer == 0)
    def _():
        xbuf[rows, :] = x_ref[...]

    x_bf = xbuf[rows, :]
    xs_o[0] = x_bf
    x = x_bf.astype(F32)
    normed = (x * inv_rms(x)).astype(BF)
    q_o[0] = mm(normed, wq[0]).astype(BF)
    k_o[0] = mm(normed, wk[0]).astype(BF)
    v_o[0] = mm(normed, wv[0]).astype(BF)

    def attend(s, carry):
        sl = pl.ds(pl.multiple_of(s * SEQ, SEQ), SEQ)
        for p in range(pairs):
            lanes = slice(p * PAIR, (p + 1) * PAIR)
            st = mm(k_o[0, sl, lanes], stack_heads(q_o[0, sl, lanes]), 1, 1)
            top = jnp.max(st, axis=0, keepdims=True)
            e = jnp.exp2((st - top) * (SCALE * LOG2E))
            prob = (e * (1.0 / jnp.sum(e, axis=0, keepdims=True))).astype(BF)
            p_o[0, pl.ds(pl.multiple_of((s * pairs + p) * SEQ, SEQ), SEQ), :] = prob
            mix_o[0, sl, lanes] = mm(rows_of(prob), stack_heads(v_o[0, sl, lanes]), 0, 0).astype(BF)
        return carry

    lax.fori_loop(0, tb // SEQ, attend, 0)
    hid = (x + mm(mix_o[0], wo[0]).astype(BF).astype(F32)).astype(BF)
    hid_o[0] = hid
    h = hid.astype(F32)
    n2 = (h * inv_rms(h)).astype(BF)
    n2_o[0] = n2
    ff = w1.shape[1]
    step = 768
    for j in range(ff // step):
        cols = slice(j * step, (j + 1) * step)
        pre = mm(n2, w1[:, cols]).astype(BF)
        pre_o[0, :, cols] = pre
        act_o[0, :, cols] = gelu(pre.astype(F32)).astype(BF)

    @pl.when(layer < layers - 1)
    def _():
        out = mm(act_o[0], w2[...]).astype(BF).astype(F32)
        xbuf[rows, :] = (hid_o[0].astype(F32) + out).astype(BF)


def forward(x, wq, wk, wv, wo, w1, w2, tb=512):
    layers, d, _ = wq.shape
    ff = w1.shape[1]
    t = x.shape[0]
    nb = t // tb
    prow = (tb // SEQ) * (d // PAIR) * SEQ
    wspec = pl.BlockSpec((1, d, d), lambda l, b: (l, 0, 0))
    once = pl.Buffered(1)

    def tok(w):
        return pl.BlockSpec((1, tb, w), lambda l, b: (l, b, 0))

    def sds(w):
        return jax.ShapeDtypeStruct((layers, t, w), BF)


    return pl.pallas_call(
        functools.partial(fwd_body, layers=layers, tb=tb),
        grid=(layers, nb),
        in_specs=[pl.BlockSpec((tb, d), lambda l, b: (jnp.where(l == 0, b, nb - 1), 0)), wspec, wspec, wspec, wspec,
                  pl.BlockSpec((d, ff), lambda l, b: (0, 0), pipeline_mode=once),
                  pl.BlockSpec((ff, d), lambda l, b: (0, 0), pipeline_mode=once)],
        out_specs=[tok(d), tok(d), tok(d), tok(d), pl.BlockSpec((1, prow, 2 * SEQ), lambda l, b: (l, b, 0)),
                   tok(d), tok(d), tok(d), tok(ff), tok(ff)],
        out_shape=[sds(d), sds(d), sds(d), sds(d), jax.ShapeDtypeStruct((layers, nb * prow, 2 * SEQ), BF),
                   sds(d), sds(d), sds(d), sds(ff), sds(ff)],
        scratch_shapes=[pltpu.VMEM((t, d), BF)],
        compiler_params=pltpu.CompilerParams(dimension_semantics=("arbitrary", "arbitrary"), vmem_limit_bytes=63 * 1024 * 1024),
        name="fwd_stack",
    )(x, wq, wk, wv, wo, w1, w2)


def rms_pull(v, dy):
    r = inv_rms(v)
    return dy * r - v * (r * r * r * jnp.mean(v * dy, axis=-1, keepdims=True))


def gelu_pull(x, d):
    sq = x * x
    t = jnp.tanh(x * (GC + (GC * GA) * sq))
    return d * (0.5 + 0.5 * t + (0.5 * x) * (1.0 - t * t) * (GC + (3.0 * GC * GA) * sq))


def bwd_body(dn_ref, x_ref, q_ref, k_ref, v_ref, p_ref, mix_ref, hid_ref, pre_ref, wq, wk, wv, wo, w1, w2,
             dx_o, keep_o, dpre_o, g_o, dmix, dq, dk, dv):
    @pl.when(pl.program_id(0) == 0)
    def _():
        g_o[...] = jnp.zeros_like(g_o)

    tb, d = dx_o.shape
    pairs = d // PAIR
    dn = dn_ref[...]
    keep_o[0] = dn
    ff = w1.shape[1]
    step = 768
    for j in range(ff // step):
        cols = slice(j * step, (j + 1) * step)
        d_act = mm(dn, w2[cols, :], 1, 1).astype(BF).astype(F32)
        dpre_o[0, :, cols] = gelu_pull(pre_ref[0, :, cols].astype(F32), d_act).astype(BF)
    d_n2 = mm(dpre_o[0], w1[...], 1, 1).astype(BF).astype(F32)
    dh = (dn.astype(F32) + rms_pull(hid_ref[0].astype(F32), d_n2)).astype(BF)
    dmix[...] = mm(dh, wo[0], 1, 1).astype(BF)
    g_o[3] += mm(mix_ref[0], dh, 0, 0)

    def attend(s, carry):
        sl = pl.ds(pl.multiple_of(s * SEQ, SEQ), SEQ)
        for p in range(pairs):
            lanes = slice(p * PAIR, (p + 1) * PAIR)
            prob = p_ref[0, pl.ds(pl.multiple_of((s * pairs + p) * SEQ, SEQ), SEQ), :]
            d_mixed = stack_heads(dmix[sl, lanes])
            d_prob = mm(v_ref[0, sl, lanes], d_mixed, 1, 1).astype(BF).astype(F32)
            dv[sl, lanes] = mm(prob, d_mixed, 1, 0).astype(BF)
            prob = prob.astype(F32)
            row = jnp.sum(d_prob * prob, axis=0, keepdims=True)
            d_st = (prob * (d_prob - row) * SCALE).astype(BF)
            dk[sl, lanes] = mm(d_st, stack_heads(q_ref[0, sl, lanes]), 1, 0).astype(BF)
            dq[sl, lanes] = mm(rows_of(d_st), stack_heads(k_ref[0, sl, lanes]), 0, 0).astype(BF)
        return carry

    lax.fori_loop(0, tb // SEQ, attend, 0)
    x = x_ref[0].astype(F32)
    normed = (x * inv_rms(x)).astype(BF)
    g_o[0] += mm(normed, dq[...], 0, 0)
    g_o[1] += mm(normed, dk[...], 0, 0)
    g_o[2] += mm(normed, dv[...], 0, 0)
    d_n1 = (mm(dq[...], wq[0], 1, 1) + mm(dk[...], wk[0], 1, 1) + mm(dv[...], wv[0], 1, 1)).astype(BF).astype(F32)
    dx_o[...] = (dh.astype(F32) + rms_pull(x, d_n1)).astype(BF)


def backward(layer, d_next, xs, q, k, v, p, mix, hid, pre, wq, wk, wv, wo, w1, w2, tb=256):
    layers, d, _ = wq.shape
    ff = w1.shape[1]
    t = d_next.shape[0]
    prow = (tb // SEQ) * (d // PAIR) * SEQ
    once = pl.Buffered(1)
    wspec = pl.BlockSpec((1, d, d), lambda b: (layer, 0, 0), pipeline_mode=once)
    flat = pl.BlockSpec((tb, d), lambda b: (b, 0))

    def tok(w):
        return pl.BlockSpec((1, tb, w), lambda b: (layer, b, 0))

    return pl.pallas_call(
        bwd_body,
        grid=(t // tb,),
        in_specs=[flat, tok(d), tok(d), tok(d), tok(d), pl.BlockSpec((1, prow, 2 * SEQ), lambda b: (layer, b, 0)),
                  tok(d), tok(d), tok(ff), wspec, wspec, wspec, wspec,
                  pl.BlockSpec((d, ff), lambda b: (0, 0), pipeline_mode=once),
                  pl.BlockSpec((ff, d), lambda b: (0, 0), pipeline_mode=once)],
        out_specs=[flat, tok(d), tok(ff), pl.BlockSpec((4, d, d), lambda b: (0, 0, 0), pipeline_mode=once)],
        out_shape=[jax.ShapeDtypeStruct((t, d), BF), jax.ShapeDtypeStruct(xs.shape, BF), jax.ShapeDtypeStruct(pre.shape, BF),
                   jax.ShapeDtypeStruct((4, d, d), F32)],
        input_output_aliases={1: 1, 8: 2},
        scratch_shapes=[pltpu.VMEM((tb, d), BF)] * 4,
        cost_estimate=pl.CostEstimate(flops=80 * 10 ** 9, transcendentals=0, bytes_accessed=150 * 10 ** 6),
        compiler_params=pltpu.CompilerParams(dimension_semantics=("arbitrary",), vmem_limit_bytes=63 * 1024 * 1024),
        name="bwd_layer",
    )(d_next, xs, q, k, v, p, mix, hid, pre, wq, wk, wv, wo, w1, w2)


def local_step(x_init, cot_out, w_query, w_key, w_value, w_proj, w_up, w_down):
    layers, width, _ = w_query.shape
    x = x_init.reshape(-1, width)
    weights = (w_query, w_key, w_value, w_proj, w_up, w_down)
    xs, q, k, v, p, mix, hid, n2, pre, act = forward(x, *weights)
    d_act = cot_out.reshape(-1, width)
    sums = [None] * layers
    last = None
    for layer in reversed(range(layers)):
        d_act, xs, pre, part = backward(layer, d_act, xs, q, k, v, p, mix, hid, pre, *weights)
        if last is not None:
            part, last = lax.optimization_barrier((part, last))
            sums[layer + 1] = last
        last = lax.psum(part, "data")
    tall = lambda a: a.reshape(-1, a.shape[-1])
    g_up = mm(tall(n2), tall(pre), 0, 0)
    g_up, last = lax.optimization_barrier((g_up, last))
    sums[0] = last
    g_up = lax.psum(g_up, "data")
    g_down = mm(tall(act), tall(xs), 0, 0)
    g_down, g_up = lax.optimization_barrier((g_down, g_up))
    g_down = lax.psum(g_down, "data")
    attn = [jnp.stack([part[i] for part in sums]) for i in range(4)]
    return (*attn, g_up, g_down, d_act.reshape(x_init.shape))


def solution(mesh):
    data_spec = P("data")
    full_spec = P()
    in_specs = (data_spec, data_spec) + (full_spec,) * 6
    out_specs = (full_spec,) * 6 + (data_spec,)
    return jax.shard_map(local_step, mesh=mesh, in_specs=in_specs, out_specs=out_specs, check_vma=False)
```

```python
import functools

import jax
import jax.numpy as jnp
from jax import lax
from jax.experimental import pallas as pl
from jax.experimental.pallas import tpu as pltpu
from jax.sharding import PartitionSpec as P

EPS = 1e-6
HEAD_DIM = 64
BF = jnp.bfloat16
F32 = jnp.float32
SEQ = 128
PAIR = 2 * HEAD_DIM
SCALE = HEAD_DIM ** -0.5
LOG2E = 1.4426950408889634
GC = 0.7978845608028654
GA = 0.044715
FWD_CHUNK = 512
BWD_CHUNK = 768


def mm(a, b, ca=1, cb=0):
    return lax.dot_general(a, b, (((ca,), (cb,)), ((), ())), preferred_element_type=F32)


def inv_rms(v):
    return lax.rsqrt(jnp.mean(v * v, axis=-1, keepdims=True) + EPS)


def stack_heads(val):
    lane = lax.broadcasted_iota(jnp.int32, val.shape, 1)
    zero = jnp.zeros_like(val)
    return jnp.concatenate([jnp.where(lane < HEAD_DIM, val, zero), jnp.where(lane < HEAD_DIM, zero, val)], axis=0)


def rows_of(val):
    return jnp.concatenate([val[:, :SEQ], val[:, SEQ:]], axis=0)


def gelu(x):
    t = jnp.tanh(x * (GC + (GC * GA) * (x * x)))
    h = 0.5 * x
    return h + h * t


def fwd_body(x_ref, wq, wk, wv, wo, w1, w2, xs_o, q_o, k_o, v_o, p_o, mix_o, hid_o, n2_o, pre_o, act_o, xbuf, mixbuf, *, layers, nb, tb):
    s = pl.program_id(0)
    cur = jnp.minimum(s, layers * nb - 1)
    old = jnp.maximum(s - 1, 0)
    rows = pl.ds(pl.multiple_of((cur % nb) * tb, tb), tb)
    rows_old = pl.ds(pl.multiple_of((old % nb) * tb, tb), tb)
    pairs = q_o.shape[-1] // PAIR

    @pl.when(s < nb)
    def _():
        xbuf[rows, :] = x_ref[...]

    @pl.when(s == 0)
    def _():
        mixbuf[...] = jnp.zeros_like(mixbuf)

    hid = (xbuf[rows_old, :].astype(F32) + mm(mixbuf[...], wo[0]).astype(BF).astype(F32)).astype(BF)
    hid_o[0] = hid
    x_bf = xbuf[rows, :]
    xs_o[0] = x_bf
    x = x_bf.astype(F32)
    normed = (x * inv_rms(x)).astype(BF)
    q_o[0] = mm(normed, wq[0]).astype(BF)
    k_o[0] = mm(normed, wk[0]).astype(BF)
    v_o[0] = mm(normed, wv[0]).astype(BF)
    h = hid.astype(F32)
    n2_o[0] = (h * inv_rms(h)).astype(BF)

    units = [(i, p) for i in range(tb // SEQ) for p in range(pairs)]
    ff = w1.shape[1]
    step = FWD_CHUNK
    chunks = ff // step
    each = -(-len(units) // chunks)

    def score(i, p):
        lanes = slice(p * PAIR, (p + 1) * PAIR)
        sl = slice(i * SEQ, (i + 1) * SEQ)
        return mm(k_o[0, sl, lanes], stack_heads(q_o[0, sl, lanes]), 1, 1)

    def soft(i, p, st):
        top = jnp.max(st, axis=0, keepdims=True)
        e = jnp.exp2((st - top) * (SCALE * LOG2E))
        prob = (e * (1.0 / jnp.sum(e, axis=0, keepdims=True))).astype(BF)
        at = (i * pairs + p) * SEQ
        p_o[0, at:at + SEQ, :] = prob
        return prob

    def mixed(i, p, prob):
        lanes = slice(p * PAIR, (p + 1) * PAIR)
        sl = slice(i * SEQ, (i + 1) * SEQ)
        val = mm(rows_of(prob), stack_heads(v_o[0, sl, lanes]), 0, 0).astype(BF)
        mix_o[0, sl, lanes] = val
        mixbuf[sl, lanes] = val

    ready = []
    for j in range(chunks):
        group = units[j * each:(j + 1) * each]
        scores = [score(*u) for u in group]
        for u, prob in ready:
            mixed(*u, prob)
        cols = slice(j * step, (j + 1) * step)
        pre = mm(n2_o[0], w1[:, cols]).astype(BF)
        pre_o[0, :, cols] = pre
        ready = [(u, soft(*u, st)) for u, st in zip(group, scores)]
        act_o[0, :, cols] = gelu(pre.astype(F32)).astype(BF)
    for u, prob in ready:
        mixed(*u, prob)

    @pl.when((s > 0) & (old < (layers - 1) * nb))
    def _():
        out = mm(act_o[0], w2[...]).astype(BF).astype(F32)
        xbuf[rows_old, :] = (hid_o[0].astype(F32) + out).astype(BF)


def forward(x, wq, wk, wv, wo, w1, w2, tb=512):
    layers, d, _ = wq.shape
    ff = w1.shape[1]
    t = x.shape[0]
    nb = t // tb
    n = layers * nb
    prow = (tb // SEQ) * (d // PAIR) * SEQ
    once = pl.Buffered(1)

    def cur(s):
        return jnp.minimum(s, n - 1)

    def old(s):
        return jnp.maximum(s - 1, 0)

    def weight(at):
        return pl.BlockSpec((1, d, d), lambda s: (at(s) // nb, 0, 0))

    def tok(w, at, r=tb):
        return pl.BlockSpec((1, r, w), lambda s: (at(s) // nb, at(s) % nb, 0))

    def sds(w):
        return jax.ShapeDtypeStruct((layers, t, w), BF)

    return pl.pallas_call(
        functools.partial(fwd_body, layers=layers, nb=nb, tb=tb),
        grid=(n + 1,),
        in_specs=[pl.BlockSpec((tb, d), lambda s: (jnp.minimum(s, nb - 1), 0)), weight(cur), weight(cur), weight(cur), weight(old),
                  pl.BlockSpec((d, ff), lambda s: (0, 0), pipeline_mode=once),
                  pl.BlockSpec((ff, d), lambda s: (0, 0), pipeline_mode=once)],
        out_specs=[tok(d, cur), tok(d, cur), tok(d, cur), tok(d, cur), tok(2 * SEQ, cur, prow),
                   tok(d, cur), tok(d, old), tok(d, old), tok(ff, old), tok(ff, old)],
        out_shape=[sds(d), sds(d), sds(d), sds(d), jax.ShapeDtypeStruct((layers, nb * prow, 2 * SEQ), BF),
                   sds(d), sds(d), sds(d), sds(ff), sds(ff)],
        scratch_shapes=[pltpu.VMEM((t, d), BF), pltpu.VMEM((tb, d), BF)],
        compiler_params=pltpu.CompilerParams(dimension_semantics=("arbitrary",), vmem_limit_bytes=63 * 1024 * 1024),
        name="fwd_stack",
    )(x, wq, wk, wv, wo, w1, w2)


def rms_pull(v, dy):
    r = inv_rms(v)
    return dy * r - v * (r * r * r * jnp.mean(v * dy, axis=-1, keepdims=True))


def gelu_pull(x, d):
    sq = x * x
    t = jnp.tanh(x * (GC + (GC * GA) * sq))
    return d * (0.5 + 0.5 * t + (0.5 * x) * (1.0 - t * t) * (GC + (3.0 * GC * GA) * sq))


def bwd_body(dn_ref, hid_ref, pre_ref, x_ref, q_ref, k_ref, v_ref, p_ref, mix_ref, wq, wk, wv, wo, w1, w2,
             dx_o, keep_o, dpre_o, g_o, dhbuf, dmix, dq, dk, dv):
    @pl.when(pl.program_id(0) == 0)
    def _():
        g_o[...] = jnp.zeros_like(g_o)
        dhbuf[...] = jnp.zeros_like(dhbuf)
        dmix[...] = jnp.zeros_like(dmix)

    tb, d = dx_o.shape
    pairs = d // PAIR
    dn = dn_ref[...]
    keep_o[0] = dn
    hid = hid_ref[0].astype(F32)
    ff = w1.shape[1]
    step = BWD_CHUNK
    chunks = ff // step
    units = [(i, p) for i in range(tb // SEQ) for p in range(pairs)]
    each = -(-len(units) // chunks)

    def place(i, p):
        return slice(i * SEQ, (i + 1) * SEQ), slice(p * PAIR, (p + 1) * PAIR), (i * pairs + p) * SEQ

    def first(i, p):
        sl, lanes, at = place(i, p)
        d_mixed = stack_heads(dmix[sl, lanes])
        d_prob = mm(v_ref[0, sl, lanes], d_mixed, 1, 1)
        dv[sl, lanes] = mm(p_ref[0, at:at + SEQ, :], d_mixed, 1, 0).astype(BF)
        return d_prob

    def soft(i, p, d_prob):
        at = place(i, p)[2]
        d_prob = d_prob.astype(BF).astype(F32)
        prob = p_ref[0, at:at + SEQ, :].astype(F32)
        row = jnp.sum(d_prob * prob, axis=0, keepdims=True)
        return (prob * (d_prob - row) * SCALE).astype(BF)

    def second(i, p, d_st):
        sl, lanes, _ = place(i, p)
        dk[sl, lanes] = mm(d_st, stack_heads(q_ref[0, sl, lanes]), 1, 0).astype(BF)
        dq[sl, lanes] = mm(rows_of(d_st), stack_heads(k_ref[0, sl, lanes]), 0, 0).astype(BF)

    ready = []
    for j in range(chunks):
        group = units[j * each:(j + 1) * each]
        scores = [first(*u) for u in group]
        for u, d_st in ready:
            second(*u, d_st)
        cols = slice(j * step, (j + 1) * step)
        d_act = mm(dn, w2[cols, :], 1, 1)
        ready = [(u, soft(*u, d_prob)) for u, d_prob in zip(group, scores)]
        dpre_o[0, :, cols] = gelu_pull(pre_ref[0, :, cols].astype(F32), d_act.astype(BF).astype(F32)).astype(BF)
    for u, d_st in ready:
        second(*u, d_st)
    dh = dhbuf[...]
    g_o[3] += mm(mix_ref[0], dh, 0, 0)
    d_n2 = mm(dpre_o[0], w1[...], 1, 1).astype(BF).astype(F32)
    x = x_ref[0].astype(F32)
    normed = (x * inv_rms(x)).astype(BF)
    g_o[0] += mm(normed, dq[...], 0, 0)
    g_o[1] += mm(normed, dk[...], 0, 0)
    g_o[2] += mm(normed, dv[...], 0, 0)
    dh_new = (dn.astype(F32) + rms_pull(hid, d_n2)).astype(BF)
    d_n1 = (mm(dq[...], wq[0], 1, 1) + mm(dk[...], wk[0], 1, 1) + mm(dv[...], wv[0], 1, 1)).astype(BF).astype(F32)
    dx_o[...] = (dh.astype(F32) + rms_pull(x, d_n1)).astype(BF)
    dmix[...] = mm(dh_new, wo[0], 1, 1).astype(BF)
    dhbuf[...] = dh_new


def backward(layer, d_next, xs, q, k, v, p, mix, hid, pre, wq, wk, wv, wo, w1, w2, tb=256):
    layers, d, _ = wq.shape
    ff = w1.shape[1]
    t = d_next.shape[0]
    nb = t // tb
    prow = (tb // SEQ) * (d // PAIR) * SEQ
    once = pl.Buffered(1)
    wspec = pl.BlockSpec((1, d, d), lambda b: (layer, 0, 0), pipeline_mode=once)

    def cur(b):
        return jnp.minimum(b, nb - 1)

    def old(b):
        return jnp.maximum(b - 1, 0)

    def tok(w, at, r=tb):
        return pl.BlockSpec((1, r, w), lambda b: (layer, at(b), 0))

    def flat(at):
        return pl.BlockSpec((tb, d), lambda b: (at(b), 0))

    return pl.pallas_call(
        bwd_body,
        grid=(nb + 1,),
        in_specs=[flat(cur), tok(d, cur), tok(ff, cur), tok(d, old), tok(d, old), tok(d, old), tok(d, old), tok(2 * SEQ, old, prow),
                  tok(d, old), wspec, wspec, wspec, wspec,
                  pl.BlockSpec((d, ff), lambda b: (0, 0), pipeline_mode=once),
                  pl.BlockSpec((ff, d), lambda b: (0, 0), pipeline_mode=once)],
        out_specs=[flat(old), tok(d, cur), tok(ff, cur), pl.BlockSpec((4, d, d), lambda b: (0, 0, 0), pipeline_mode=once)],
        out_shape=[jax.ShapeDtypeStruct((t, d), BF), jax.ShapeDtypeStruct(hid.shape, BF), jax.ShapeDtypeStruct(pre.shape, BF),
                   jax.ShapeDtypeStruct((4, d, d), F32)],
        input_output_aliases={1: 1, 2: 2},
        scratch_shapes=[pltpu.VMEM((tb, d), BF)] * 5,
        cost_estimate=pl.CostEstimate(flops=80 * 10 ** 9, transcendentals=0, bytes_accessed=150 * 10 ** 6),
        compiler_params=pltpu.CompilerParams(dimension_semantics=("arbitrary",), vmem_limit_bytes=63 * 1024 * 1024),
        name="bwd_layer",
    )(d_next, hid, pre, xs, q, k, v, p, mix, wq, wk, wv, wo, w1, w2)


def local_step(x_init, cot_out, w_query, w_key, w_value, w_proj, w_up, w_down):
    layers, width, _ = w_query.shape
    x = x_init.reshape(-1, width)
    weights = (w_query, w_key, w_value, w_proj, w_up, w_down)
    xs, q, k, v, p, mix, hid, n2, pre, act = forward(x, *weights)
    d_act = cot_out.reshape(-1, width)
    sums = [None] * layers
    last = None
    for layer in reversed(range(layers)):
        d_act, hid, pre, part = backward(layer, d_act, xs, q, k, v, p, mix, hid, pre, *weights)
        if last is not None:
            part, last = lax.optimization_barrier((part, last))
            sums[layer + 1] = last
        last = lax.psum(part, "data")
    tall = lambda a: a.reshape(-1, a.shape[-1])
    g_up = mm(tall(n2), tall(pre), 0, 0)
    g_up, last = lax.optimization_barrier((g_up, last))
    sums[0] = last
    g_up = lax.psum(g_up, "data")
    g_down = mm(tall(act), tall(hid), 0, 0)
    g_down, g_up = lax.optimization_barrier((g_down, g_up))
    g_down = lax.psum(g_down, "data")
    attn = [jnp.stack([part[i] for part in sums]) for i in range(4)]
    return (*attn, g_up, g_down, d_act.reshape(x_init.shape))


def solution(mesh):
    data_spec = P("data")
    full_spec = P()
    in_specs = (data_spec, data_spec) + (full_spec,) * 6
    out_specs = (full_spec,) * 6 + (data_spec,)
    return jax.shard_map(local_step, mesh=mesh, in_specs=in_specs, out_specs=out_specs, check_vma=False)
```
